32 devices in a mesh: copy: 2 (over core), shard: 4 (over y, x), cols: 4 (over z).
Axes of the slice: x: 2, y: 2, z: 4, core: 2. Of those that a mesh axis runs over, the one named last changes fastest.
Arguments:
- train_gate: float32 [5120, 9728], P(('copy', 'shard'), 'cols'), parts along dimension 0, may hold values from -0.15625 to 0.15625
- drift_gate: float32 [5120, 9728], P(('copy', 'shard'), 'cols'), parts along dimension 0, may hold values from -6 to 6
- spread_gate: float32 [5120, 9728], P(('copy', 'shard'), 'cols'), parts along dimension 0, may hold values from 0.1 to 10
- train_up: float32 [5120, 9728], P(('copy', 'shard'), 'cols'), parts along dimension 0, may hold values from -0.15625 to 0.15625
- drift_up: float32 [5120, 9728], P(('copy', 'shard'), 'cols'), parts along dimension 0, may hold values from -6 to 6
- spread_up: float32 [5120, 9728], P(('copy', 'shard'), 'cols'), parts along dimension 0, may hold values from 0.1 to 10
- norm_train: float32 [5120], P(('copy', 'shard', 'cols')), parts along dimension 0, may hold values from 0.25 to 1.75
- norm_step: float32 [5120], P(('copy', 'shard', 'cols')), parts along dimension 0, may hold values from -0.3 to 0.3
Outputs:
- final_gate: bfloat16 [5120, 9728], P('copy', 'cols'), parts along dimension 0
- final_up: bfloat16 [5120, 9728], P('copy', 'cols'), parts along dimension 0
- column_gate: float32 [19456], P(('copy', 'cols')), parts along dimension 0
- column_up: float32 [19456], P(('copy', 'cols')), parts along dimension 0
- serve_norm: bfloat16 [5120], P('copy'), parts along dimension 0
- result_gate: float32 [5120, 9728], P(('copy', 'shard'), 'cols'), parts along dimension 0
- result_up: float32 [5120, 9728], P(('copy', 'shard'), 'cols'), parts along dimension 0
The draws below stay inside these ranges and needn't reach their ends.
There are 2 independent parts, one for each index of `copy`. The reference program is written for one: setup_inputs(seed, part) draws one part's arguments, and reference() takes and returns one part's arrays. A program takes and returns all parts, laid end to end along the dimension named above; each array names one. Nothing has to cross between parts.
All inputs are finite; a program needn't handle non-finite values.
Results may differ from the reference program's by a relative error of at most 0.0004.
Values may be sent and summed in bfloat16 or wider, within the bound.
A program may use at most 192 MiB of HBM per device.

```python
import math
import jax
import jax.numpy as jnp
from jax import lax

D_MODEL = 2560
D_INNER = 9728


def strengthened(array, rng, source, target, blocks, factor):
    owner, partner = [(jnp.arange(array.shape[position]) // (array.shape[position] // blocks)).reshape([-1 if axis == position else 1 for axis in range(array.ndim)]) for position in (source, target)]
    chosen = jax.random.permutation(rng, blocks)[partner]
    strong = (owner == chosen) | (owner == (partner + blocks // 2) % blocks)
    return jnp.where(strong, factor * array, array)


def block_scale(own_key, shape, shards, low, high):
    def one(dim, shards_of):
        draws = jax.random.uniform(jax.random.fold_in(jax.random.fold_in(own_key, 6), dim), (shards_of,), jnp.float32, low / len(shards), high / len(shards))
        return jnp.repeat(jnp.exp(draws), shape[dim] // shards_of).reshape((-1,) + (1,) * (len(shape) - dim - 1))

    factor_of = one(*shards[0])
    for cut in shards[1:]:
        factor_of = factor_of * one(*cut)
    return factor_of


def gaussian(stream_key, shape, scale, most, cuts=(), kind=jnp.bfloat16):
    factor_of = block_scale(stream_key, shape, cuts, -0.22, 0.18) if cuts else 1.0
    drawn = jax.random.normal(stream_key, shape, jnp.float32) * scale * factor_of
    return jnp.minimum(jnp.maximum(drawn, -most), most).astype(kind)


def gaussian_with(stream_key, extent, deviation, bound, cuts, heavy, kind=jnp.bfloat16):
    values = deviation * jax.random.normal(stream_key, extent, jnp.float32)
    if cuts:
        values = values * block_scale(stream_key, extent, cuts, -0.22, 0.18)
    return jnp.clip(strengthened(values, jax.random.fold_in(stream_key, 3), *heavy), -bound, bound).astype(kind)


def setup_inputs(seed: int = 0, part: int = 0) -> dict:
    arg_keys = jax.random.split(jax.random.key(seed), 9)
    part_keys = jax.random.split(jax.random.fold_in(arg_keys[8], part), 9)
    train_gate = gaussian_with(part_keys[0], (D_MODEL, D_INNER), D_MODEL ** -0.5, 0.15625, ((0, 4), (1, 4)), (0, 1, 4, 2.0), jnp.float32)
    drift_gate = gaussian(part_keys[1], (D_MODEL, D_INNER), 1.0, 6.0, ((0, 4), (1, 4)), jnp.float32)
    spread_gate = jnp.clip(jnp.exp(math.log(10.0) - 4.6051702 * jax.random.uniform(part_keys[2], (D_MODEL, D_INNER), jnp.float32) ** block_scale(part_keys[2], (D_MODEL, D_INNER), ((0, 4), (1, 4)), -0.2, 0.2)), 0.1, 10.0)
    train_up = gaussian_with(part_keys[3], (D_MODEL, D_INNER), D_MODEL ** -0.5, 0.15625, ((0, 4), (1, 4)), (0, 1, 4, 2.0), jnp.float32)
    drift_up = gaussian(part_keys[4], (D_MODEL, D_INNER), 1.0, 6.0, ((0, 4), (1, 4)), jnp.float32)
    spread_up = jnp.clip(jnp.exp(math.log(10.0) - 4.6051702 * jax.random.uniform(part_keys[5], (D_MODEL, D_INNER), jnp.float32) ** block_scale(part_keys[5], (D_MODEL, D_INNER), ((0, 4), (1, 4)), -0.2, 0.2)), 0.1, 10.0)
    norm_train = jnp.clip(1.0 + 0.15 * jax.random.normal(part_keys[6], (D_MODEL,), jnp.float32), 0.25, 1.75)
    norm_step = jnp.clip(jax.random.uniform(part_keys[7], (D_MODEL,), jnp.float32, -0.3, 0.3) * block_scale(part_keys[7], (D_MODEL,), ((0, 16),), -0.4, 0.0), -0.3, 0.3)
    return {"train_gate": train_gate, "drift_gate": drift_gate, "spread_gate": spread_gate, "train_up": train_up, "drift_up": drift_up, "spread_up": spread_up, "norm_train": norm_train, "norm_step": norm_step}


learn_rate = 0.015
decay_rate = 0.1
tiny_value = 1e-08

def reference(train_gate, drift_gate, spread_gate, train_up, drift_up, spread_up, norm_train, norm_step):
    result_gate = train_gate - learn_rate * (drift_gate / (jnp.sqrt(spread_gate) + tiny_value) + decay_rate * train_gate)
    result_up = train_up - learn_rate * (drift_up / (jnp.sqrt(spread_up) + tiny_value) + decay_rate * train_up)
    column_gate = jnp.sqrt(lax.optimization_barrier(jnp.sum(result_gate * result_gate, axis=0)))
    final_gate = (result_gate / column_gate).astype(jnp.bfloat16)
    column_up = jnp.sqrt(lax.optimization_barrier(jnp.sum(result_up * result_up, axis=0)))
    final_up = (result_up / column_up).astype(jnp.bfloat16)
    serve_norm = (norm_train + norm_step).astype(jnp.bfloat16)
    return (final_gate, final_up, column_gate, column_up, serve_norm, result_gate, result_up)
```

```python
import functools

import jax
import jax.numpy as jnp
from jax import lax
from jax.experimental import pallas as pl
from jax.experimental.pallas import tpu as pltpu
from jax.sharding import PartitionSpec as P

learn_rate = 0.015
decay_rate = 0.1
tiny_value = 1e-08
LANES = 128
BLOCK = 64
LAG = 3
MESH = pl.DeviceIdType.MESH


def stepped(train, drift, spread):
    return train - learn_rate * (
        drift / (jnp.sqrt(spread) + tiny_value) + decay_rate * train
    )


def plain(
    train_gate, drift_gate, spread_gate, train_up, drift_up, spread_up, norm_train, norm_step
):
    result_gate = stepped(train_gate, drift_gate, spread_gate)
    result_up = stepped(train_up, drift_up, spread_up)
    total_gate, total_up = lax.psum(
        (jnp.sum(result_gate * result_gate, axis=0), jnp.sum(result_up * result_up, axis=0)),
        "shard",
    )
    column_gate = jnp.sqrt(total_gate)
    column_up = jnp.sqrt(total_up)
    narrow_gate = (result_gate / column_gate).astype(jnp.bfloat16)
    narrow_up = (result_up / column_up).astype(jnp.bfloat16)
    final_gate = lax.all_gather(narrow_gate, "shard", axis=0, tiled=True)
    final_up = lax.all_gather(narrow_up, "shard", axis=0, tiled=True)
    serve_norm = lax.all_gather(
        (norm_train + norm_step).astype(jnp.bfloat16), ("shard", "cols"), axis=0, tiled=True
    )
    return (final_gate, final_up, column_gate, column_up, serve_norm, result_gate, result_up)


def gather_kernel(
    chunks, ncols,
    tg, dg, sg, tu, du, su, norm_a, norm_b,
    T, R, col, N,
    inbuf, res, own, part, gain,
    in_sem, res_sem, loc_sem, psend, precv, osend, orecv, fsend, frecv, nsend, nrecv,
):
    ins = (tg, dg, sg, tu, du, su)
    rows = tg.shape[0]
    me = lax.axis_index("shard")
    mc = lax.axis_index("cols")
    mx = lax.rem(me, 2)
    my = me // 2
    nx = my * 2 + (1 - mx)
    ny = (1 - my) * 2 + mx
    nd = (1 - my) * 2 + (1 - mx)
    peers = (nx, ny, nd)

    def fetch(c, slot):
        return [
            pltpu.make_async_copy(
                ins[k].at[:, pl.ds(pl.multiple_of(c * LANES, LANES), LANES)],
                inbuf.at[slot, k],
                in_sem.at[slot, k],
            )
            for k in range(6)
        ]

    for f in fetch(0, 0):
        f.start()

    everyone = [(i, j) for i in range(4) for j in range(ncols) if i or j]

    def other(i, j):
        return {"shard": lax.rem(me + i, 4), "cols": lax.rem(mc + j, ncols)}

    barrier = pltpu.get_barrier_semaphore()
    for i, j in everyone:
        pl.semaphore_signal(barrier, inc=1, device_id=other(i, j), device_id_type=MESH)
    pl.semaphore_wait(barrier, len(everyone))

    def remote(src, dst, send, recv, shard):
        return pltpu.make_async_remote_copy(
            src_ref=src, dst_ref=dst, send_sem=send, recv_sem=recv,
            device_id={"shard": shard}, device_id_type=MESH,
        )

    def share(c, k):
        return remote(part.at[c, me], part.at[c, me], psend.at[c, k], precv.at[c, k], peers[k])

    def share_in(c, k):
        return remote(part.at[c, peers[k]], part.at[c, peers[k]], psend.at[c, k], precv.at[c, k], peers[k])

    def give(c, k):
        return remote(own.at[c], T.at[c, me], osend.at[c, k], orecv.at[c, k], peers[k])

    def give_in(c, k):
        return remote(own.at[c], T.at[c, peers[k]], osend.at[c, k], orecv.at[c, k], peers[k])

    def pass_on(c, k):
        return remote(
            T.at[c, peers[1 - k], 1 - k], T.at[c, peers[1 - k], 1 - k],
            fsend.at[c, k], frecv.at[c, k], peers[k],
        )

    def pass_in(c, k):
        return remote(
            T.at[c, nd, 1 - k], T.at[c, nd, 1 - k],
            fsend.at[c, k], frecv.at[c, k], peers[k],
        )

    def save(c):
        return pltpu.make_async_copy(res.at[c], R.at[c], res_sem.at[c])

    def keep(c):
        return pltpu.make_async_copy(own.at[c], T.at[c, me], loc_sem.at[c])

    def stage_a(c):
        slot = lax.rem(c, 2)
        for f in fetch(c, slot):
            f.wait()

        @pl.when(c + 1 < chunks)
        def _():
            for f in fetch(c + 1, 1 - slot):
                f.start()

        for g in range(2):
            def body(i, acc):
                at = pl.ds(pl.multiple_of(i * BLOCK, BLOCK), BLOCK)
                value = stepped(
                    inbuf[slot, 3 * g, at, :], inbuf[slot, 3 * g + 1, at, :], inbuf[slot, 3 * g + 2, at, :]
                )
                res[c, g, at, :] = value
                return acc + jnp.sum((value * value).reshape(BLOCK // 8, 8, LANES), axis=0)

            acc = lax.fori_loop(0, rows // BLOCK, body, jnp.zeros((8, LANES), jnp.float32))
            part[c, me, pl.ds(g, 1), :] = jnp.sum(acc, axis=0, keepdims=True)
        for k in range(3):
            share(c, k).start()
        save(c).start()

    def stage_b(c):
        for k in range(3):
            share_in(c, k).wait_recv()
        scale = jnp.sqrt(part[c, 0] + part[c, 1] + part[c, 2] + part[c, 3])
        col[c] = scale
        for g in range(2):
            divisor = scale[g : g + 1, :]

            def body(i, _):
                at = pl.ds(pl.multiple_of(i * BLOCK, BLOCK), BLOCK)
                own[c, g, at, :] = (res[c, g, at, :] / divisor).astype(jnp.bfloat16)
                return 0

            lax.fori_loop(0, rows // BLOCK, body, 0)
        for k in range(2):
            give(c, k).start()
        keep(c).start()

    def stage_c(c):
        for k in range(2):
            give_in(c, k).wait_recv()
            pass_on(c, 1 - k).start()

    stage_a(0)

    mine = me * ncols + mc
    gain[mine] = (norm_a[...] + norm_b[...]).astype(jnp.bfloat16)

    def gain_copy(n, i, j):
        to = other(i, j)
        return pltpu.make_async_remote_copy(
            src_ref=gain.at[mine], dst_ref=gain.at[mine],
            send_sem=nsend.at[n], recv_sem=nrecv.at[n], device_id=to, device_id_type=MESH,
        )

    def gain_in(n, i, j):
        source = lax.rem(me + 4 - i, 4) * ncols + lax.rem(mc + ncols - j, ncols)
        return pltpu.make_async_remote_copy(
            src_ref=gain.at[source], dst_ref=gain.at[source],
            send_sem=nsend.at[n], recv_sem=nrecv.at[n], device_id=other(i, j), device_id_type=MESH,
        )

    def step(c, _):
        @pl.when(c + 1 < chunks)
        def _():
            stage_a(c + 1)

        stage_b(c)

        @pl.when(c >= LAG)
        def _():
            stage_c(c - LAG)

        return 0

    lax.fori_loop(0, chunks, step, 0)
    for n, (i, j) in enumerate(everyone):
        gain_copy(n, i, j).start()
    lax.fori_loop(chunks - LAG, chunks, lambda c, _: (stage_c(c), 0)[1], 0)

    def finish(c, _):
        for k in range(3):
            share(c, k).wait_send()
        for k in range(2):
            give(c, k).wait_send()
            pass_on(c, k).wait_send()
            pass_in(c, k).wait_recv()
        keep(c).wait()
        save(c).wait()
        return 0

    lax.fori_loop(0, chunks, finish, 0)
    for n, (i, j) in enumerate(everyone):
        gain_copy(n, i, j).wait_send()
        gain_in(n, i, j).wait_recv()
    N[...] = gain[...]


def spread_kernel(chunks, T, R, fg, fu, rg, ru):
    for c in range(chunks):
        at = slice(c * LANES, (c + 1) * LANES)
        fg[:, at] = T[c, 0, 0]
        fu[:, at] = T[c, 0, 1]
        rg[:, at] = R[c, 0]
        ru[:, at] = R[c, 1]


def ringed(tg, dg, sg, tu, du, su, norm_train, norm_step, ncols):
    rows, width = tg.shape
    chunks = width // LANES
    small = norm_train.shape[0]
    peers = 4 * ncols - 1
    bf16, f32 = jnp.bfloat16, jnp.float32
    dma = pltpu.SemaphoreType.DMA
    any_spec = pl.BlockSpec(memory_space=pl.ANY)
    vmem = pl.BlockSpec(memory_space=pltpu.VMEM)
    T, R, col, N = pl.pallas_call(
        functools.partial(gather_kernel, chunks, ncols),
        out_shape=(
            jax.ShapeDtypeStruct((chunks, 4, 2, rows, LANES), bf16),
            jax.ShapeDtypeStruct((chunks, 2, rows, LANES), f32),
            jax.ShapeDtypeStruct((chunks, 2, LANES), f32),
            jax.ShapeDtypeStruct((4 * ncols, 1, small), bf16),
        ),
        in_specs=[any_spec] * 6 + [vmem] * 2,
        out_specs=(any_spec, any_spec, vmem, vmem),
        scratch_shapes=[
            pltpu.VMEM((2, 6, rows, LANES), f32),
            pltpu.VMEM((chunks, 2, rows, LANES), f32),
            pltpu.VMEM((chunks, 2, rows, LANES), bf16),
            pltpu.VMEM((chunks, 4, 2, LANES), f32),
            pltpu.VMEM((4 * ncols, 1, small), bf16),
            dma((2, 6)), dma((chunks,)), dma((chunks,)),
            dma((chunks, 3)), dma((chunks, 3)),
            dma((chunks, 2)), dma((chunks, 2)),
            dma((chunks, 2)), dma((chunks, 2)),
            dma((peers,)), dma((peers,)),
        ],
        compiler_params=pltpu.CompilerParams(
            collective_id=0, has_side_effects=True, vmem_limit_bytes=48 * 2**20
        ),
    )(tg, dg, sg, tu, du, su, norm_train.reshape(1, small), norm_step.reshape(1, small))

    steps = 5
    block = rows // steps
    thin = rows // (4 * steps)
    fg, fu, rg, ru = pl.pallas_call(
        functools.partial(spread_kernel, chunks),
        grid=(4, steps),
        out_shape=(
            jax.ShapeDtypeStruct((4 * rows, width), bf16),
            jax.ShapeDtypeStruct((4 * rows, width), bf16),
            jax.ShapeDtypeStruct((rows, width), f32),
            jax.ShapeDtypeStruct((rows, width), f32),
        ),
        in_specs=[
            pl.BlockSpec((chunks, 1, 2, block, LANES), lambda s, r: (0, s, 0, r, 0)),
            pl.BlockSpec((chunks, 2, thin, LANES), lambda s, r: (0, 0, s * steps + r, 0)),
        ],
        out_specs=(
            pl.BlockSpec((block, width), lambda s, r: (s * steps + r, 0)),
            pl.BlockSpec((block, width), lambda s, r: (s * steps + r, 0)),
            pl.BlockSpec((thin, width), lambda s, r: (s * steps + r, 0)),
            pl.BlockSpec((thin, width), lambda s, r: (s * steps + r, 0)),
        ),
    )(T, R)
    return (
        fg, fu, col[:, 0].reshape(width), col[:, 1].reshape(width), N.reshape(4 * ncols * small), rg, ru
    )


def solution(mesh):
    ncols = mesh.shape["cols"]

    def local(*args):
        rows, width = args[0].shape
        if mesh.shape["shard"] == 4 and width % LANES == 0 and rows % 320 == 0 and width // LANES > LAG:
            return ringed(*args, ncols)
        return plain(*args)

    return jax.shard_map(
        local,
        mesh=mesh,
        in_specs=(P(("copy", "shard"), "cols"),) * 6 + (P(("copy", "shard", "cols")),) * 2,
        out_specs=(
            P("copy", "cols"),
            P("copy", "cols"),
            P(("copy", "cols")),
            P(("copy", "cols")),
            P("copy"),
            P(("copy", "shard"), "cols"),
            P(("copy", "shard"), "cols"),
        ),
        check_vma=False,
    )
```

```python
import functools

import jax
import jax.numpy as jnp
from jax import lax
from jax.experimental import pallas as pl
from jax.experimental.pallas import tpu as pltpu
from jax.sharding import PartitionSpec as P

learn_rate = 0.015
decay_rate = 0.1
tiny_value = 1e-08
LANES = 128
BLOCK = 64
LAG = 3
TAIL = 3
MESH = pl.DeviceIdType.MESH


def stepped(train, drift, spread):
    return train - learn_rate * (
        drift / (jnp.sqrt(spread) + tiny_value) + decay_rate * train
    )


def plain(
    train_gate, drift_gate, spread_gate, train_up, drift_up, spread_up, norm_train, norm_step
):
    result_gate = stepped(train_gate, drift_gate, spread_gate)
    result_up = stepped(train_up, drift_up, spread_up)
    total_gate, total_up = lax.psum(
        (jnp.sum(result_gate * result_gate, axis=0), jnp.sum(result_up * result_up, axis=0)),
        "shard",
    )
    column_gate = jnp.sqrt(total_gate)
    column_up = jnp.sqrt(total_up)
    narrow_gate = (result_gate / column_gate).astype(jnp.bfloat16)
    narrow_up = (result_up / column_up).astype(jnp.bfloat16)
    final_gate = lax.all_gather(narrow_gate, "shard", axis=0, tiled=True)
    final_up = lax.all_gather(narrow_up, "shard", axis=0, tiled=True)
    serve_norm = lax.all_gather(
        (norm_train + norm_step).astype(jnp.bfloat16), ("shard", "cols"), axis=0, tiled=True
    )
    return (final_gate, final_up, column_gate, column_up, serve_norm, result_gate, result_up)


def gather_kernel(
    chunks, ncols,
    tg, dg, sg, tu, du, su, norm_a, norm_b,
    T, R, Og, Ou, col, N,
    inbuf, res, own, part, gain,
    in_sem, res_sem, loc_sem, tail_sem, psend, precv, osend, orecv, fsend, frecv, nsend, nrecv,
):
    ins = (tg, dg, sg, tu, du, su)
    lead = T.shape[0]
    rows = tg.shape[0]
    me = lax.axis_index("shard")
    mc = lax.axis_index("cols")
    mx = lax.rem(me, 2)
    my = me // 2
    nx = my * 2 + (1 - mx)
    ny = (1 - my) * 2 + mx
    nd = (1 - my) * 2 + (1 - mx)
    peers = (nx, ny, nd)

    def fetch(c, slot):
        return [
            pltpu.make_async_copy(
                ins[k].at[:, pl.ds(pl.multiple_of(c * LANES, LANES), LANES)],
                inbuf.at[slot, k],
                in_sem.at[slot, k],
            )
            for k in range(6)
        ]

    for f in fetch(0, 0):
        f.start()

    everyone = [(i, j) for i in range(4) for j in range(ncols) if i or j]

    def other(i, j):
        return {"shard": lax.rem(me + i, 4), "cols": lax.rem(mc + j, ncols)}

    barrier = pltpu.get_barrier_semaphore()
    for i, j in everyone:
        pl.semaphore_signal(barrier, inc=1, device_id=other(i, j), device_id_type=MESH)
    pl.semaphore_wait(barrier, len(everyone))

    def remote(src, dst, send, recv, shard):
        return pltpu.make_async_remote_copy(
            src_ref=src, dst_ref=dst, send_sem=send, recv_sem=recv,
            device_id={"shard": shard}, device_id_type=MESH,
        )

    def share(c, k):
        return remote(part.at[c, me], part.at[c, me], psend.at[c, k], precv.at[c, k], peers[k])

    def share_in(c, k):
        return remote(part.at[c, peers[k]], part.at[c, peers[k]], psend.at[c, k], precv.at[c, k], peers[k])

    def give(c, k):
        return remote(own.at[c], T.at[c, me], osend.at[c, k], orecv.at[c, k], peers[k])

    def give_in(c, k):
        return remote(own.at[c], T.at[c, peers[k]], osend.at[c, k], orecv.at[c, k], peers[k])

    def pass_on(c, k):
        return remote(
            T.at[c, peers[1 - k], 1 - k], T.at[c, peers[1 - k], 1 - k],
            fsend.at[c, k], frecv.at[c, k], peers[k],
        )

    def pass_in(c, k):
        return remote(
            T.at[c, nd, 1 - k], T.at[c, nd, 1 - k],
            fsend.at[c, k], frecv.at[c, k], peers[k],
        )

    def save(c):
        return pltpu.make_async_copy(res.at[c], R.at[c], res_sem.at[c])

    def keep(c):
        return pltpu.make_async_copy(own.at[c], T.at[c, me], loc_sem.at[c])

    def leave(c):
        return [
            pltpu.make_async_copy(own.at[lead + c, g], out.at[c], tail_sem.at[c, g])
            for g, out in enumerate((Og, Ou))
        ]

    def stage_a(c):
        slot = lax.rem(c, 2)
        for f in fetch(c, slot):
            f.wait()

        @pl.when(c + 1 < chunks)
        def _():
            for f in fetch(c + 1, 1 - slot):
                f.start()

        for g in range(2):
            def body(i, acc):
                at = pl.ds(pl.multiple_of(i * BLOCK, BLOCK), BLOCK)
                value = stepped(
                    inbuf[slot, 3 * g, at, :], inbuf[slot, 3 * g + 1, at, :], inbuf[slot, 3 * g + 2, at, :]
                )
                res[c, g, at, :] = value
                return acc + jnp.sum((value * value).reshape(BLOCK // 8, 8, LANES), axis=0)

            acc = lax.fori_loop(0, rows // BLOCK, body, jnp.zeros((8, LANES), jnp.float32))
            part[c, me, pl.ds(g, 1), :] = jnp.sum(acc, axis=0, keepdims=True)
        for k in range(3):
            share(c, k).start()
        save(c).start()

    def stage_b(c):
        for k in range(3):
            share_in(c, k).wait_recv()
        scale = jnp.sqrt(part[c, 0] + part[c, 1] + part[c, 2] + part[c, 3])
        col[c] = scale
        for g in range(2):
            divisor = scale[g : g + 1, :]

            def body(i, _):
                at = pl.ds(pl.multiple_of(i * BLOCK, BLOCK), BLOCK)
                own[c, g, at, :] = (res[c, g, at, :] / divisor).astype(jnp.bfloat16)
                return 0

            lax.fori_loop(0, rows // BLOCK, body, 0)

        @pl.when(c < lead)
        def _():
            for k in range(2):
                give(c, k).start()
            keep(c).start()

        @pl.when(c >= lead)
        def _():
            for copy in leave(c - lead):
                copy.start()

    def stage_c(c):
        for k in range(2):
            give_in(c, k).wait_recv()
            pass_on(c, 1 - k).start()

    stage_a(0)

    mine = me * ncols + mc
    gain[mine] = (norm_a[...] + norm_b[...]).astype(jnp.bfloat16)

    def gain_copy(n, i, j):
        to = other(i, j)
        return pltpu.make_async_remote_copy(
            src_ref=gain.at[mine], dst_ref=gain.at[mine],
            send_sem=nsend.at[n], recv_sem=nrecv.at[n], device_id=to, device_id_type=MESH,
        )

    def gain_in(n, i, j):
        source = lax.rem(me + 4 - i, 4) * ncols + lax.rem(mc + ncols - j, ncols)
        return pltpu.make_async_remote_copy(
            src_ref=gain.at[source], dst_ref=gain.at[source],
            send_sem=nsend.at[n], recv_sem=nrecv.at[n], device_id=other(i, j), device_id_type=MESH,
        )

    def step(c, _):
        @pl.when(c + 1 < chunks)
        def _():
            stage_a(c + 1)

        stage_b(c)

        @pl.when((c >= LAG) & (c < lead + LAG))
        def _():
            stage_c(c - LAG)

        return 0

    lax.fori_loop(0, chunks, step, 0)
    for n, (i, j) in enumerate(everyone):
        gain_copy(n, i, j).start()
    if lead > chunks - LAG:
        lax.fori_loop(chunks - LAG, lead, lambda c, _: (stage_c(c), 0)[1], 0)

    def settle(c, _):
        for k in range(3):
            share(c, k).wait_send()
        save(c).wait()
        return 0

    def finish(c, _):
        for k in range(2):
            give(c, k).wait_send()
            pass_on(c, k).wait_send()
            pass_in(c, k).wait_recv()
        keep(c).wait()
        return 0

    lax.fori_loop(0, chunks, settle, 0)
    for c in range(chunks - lead):
        for copy in leave(c):
            copy.wait()
    lax.fori_loop(0, lead, finish, 0)
    for n, (i, j) in enumerate(everyone):
        gain_copy(n, i, j).wait_send()
        gain_in(n, i, j).wait_recv()
    N[...] = gain[...]


def lead_kernel(lead, T, fg, fu):
    for c in range(lead):
        at = slice(c * LANES, (c + 1) * LANES)
        fg[:, at] = T[c, 0, 0]
        fu[:, at] = T[c, 0, 1]


def result_kernel(chunks, R, rg, ru):
    for c in range(chunks):
        at = slice(c * LANES, (c + 1) * LANES)
        rg[:, at] = R[c, 0]
        ru[:, at] = R[c, 1]


def near_kernel(place, og, ou, xg, xu, yg, yu, held_g, held_u, fg, fu):
    for j, (gate, up) in enumerate(((og, ou), (xg, xu), (yg, yu))):
        @pl.when(pl.program_id(1) == j)
        def _():
            fg[...] = gate[0]
            fu[...] = up[0]


def far_kernel(place, g, u, held_g, held_u, fg, fu):
    fg[...] = g[0]
    fu[...] = u[0]


def ringed(tg, dg, sg, tu, du, su, norm_train, norm_step, ncols):
    rows, width = tg.shape
    chunks = width // LANES
    small = norm_train.shape[0]
    peers = 4 * ncols - 1
    bf16, f32 = jnp.bfloat16, jnp.float32
    dma = pltpu.SemaphoreType.DMA
    any_spec = pl.BlockSpec(memory_space=pl.ANY)
    vmem = pl.BlockSpec(memory_space=pltpu.VMEM)
    lead = chunks - TAIL
    T, R, Og, Ou, col, N = pl.pallas_call(
        functools.partial(gather_kernel, chunks, ncols),
        out_shape=(
            jax.ShapeDtypeStruct((lead, 4, 2, rows, LANES), bf16),
            jax.ShapeDtypeStruct((chunks, 2, rows, LANES), f32),
            jax.ShapeDtypeStruct((TAIL, rows, LANES), bf16),
            jax.ShapeDtypeStruct((TAIL, rows, LANES), bf16),
            jax.ShapeDtypeStruct((chunks, 2, LANES), f32),
            jax.ShapeDtypeStruct((4 * ncols, 1, small), bf16),
        ),
        in_specs=[any_spec] * 6 + [vmem] * 2,
        out_specs=(any_spec,) * 4 + (vmem,) * 2,
        scratch_shapes=[
            pltpu.VMEM((2, 6, rows, LANES), f32),
            pltpu.VMEM((chunks, 2, rows, LANES), f32),
            pltpu.VMEM((chunks, 2, rows, LANES), bf16),
            pltpu.VMEM((chunks, 4, 2, LANES), f32),
            pltpu.VMEM((4 * ncols, 1, small), bf16),
            dma((2, 6)), dma((chunks,)), dma((lead,)), dma((TAIL, 2)),
            dma((chunks, 3)), dma((chunks, 3)),
            dma((lead, 2)), dma((lead, 2)),
            dma((lead, 2)), dma((lead, 2)),
            dma((peers,)), dma((peers,)),
        ],
        compiler_params=pltpu.CompilerParams(
            collective_id=0, has_side_effects=True, vmem_limit_bytes=48 * 2**20
        ),
    )(tg, dg, sg, tu, du, su, norm_train.reshape(1, small), norm_step.reshape(1, small))

    over_x = [(s, s ^ 1) for s in range(4)]
    over_y = [(s, s ^ 2) for s in range(4)]
    xg = lax.ppermute(Og, "shard", over_x)
    yu = lax.ppermute(Ou, "shard", over_y)
    xu = lax.ppermute(Ou, "shard", over_x)
    yg = lax.ppermute(Og, "shard", over_y)

    finals = (jax.ShapeDtypeStruct((4 * rows, width), bf16),) * 2
    results = (jax.ShapeDtypeStruct((rows, width), f32),) * 2
    steps = 5
    block = rows // steps
    cost = functools.partial(pl.CostEstimate, flops=0, transcendentals=0)
    fg, fu = pl.pallas_call(
        functools.partial(lead_kernel, lead),
        grid=(4, steps),
        out_shape=finals,
        in_specs=[pl.BlockSpec((lead, 1, 2, block, LANES), lambda s, r: (0, s, 0, r, 0))],
        out_specs=(pl.BlockSpec((block, lead * LANES), lambda s, r: (s * steps + r, 0)),) * 2,
        cost_estimate=cost(bytes_accessed=32 * lead * rows * LANES),
    )(T)
    xg, yu, fg, fu = lax.optimization_barrier((xg, yu, fg, fu))
    far_g = lax.ppermute(xg, "shard", over_y)
    far_u = lax.ppermute(yu, "shard", over_x)
    thin = rows // 10
    rg, ru = pl.pallas_call(
        functools.partial(result_kernel, chunks),
        grid=(10,),
        out_shape=results,
        in_specs=[pl.BlockSpec((chunks, 2, thin, LANES), lambda r: (0, 0, r, 0))],
        out_specs=(pl.BlockSpec((thin, width), lambda r: (r, 0)),) * 2,
        cost_estimate=cost(bytes_accessed=16 * rows * width),
    )(R)

    me = lax.axis_index("shard")
    place = jnp.stack([me, me ^ 1, me ^ 2, me ^ 3]).astype(jnp.int32)
    piece = pl.BlockSpec((1, rows, LANES), lambda c, j, p: (c, 0, 0))
    fg, fu = pl.pallas_call(
        near_kernel,
        grid_spec=pltpu.PrefetchScalarGridSpec(
            num_scalar_prefetch=1,
            grid=(TAIL, 3),
            in_specs=[piece] * 6 + [any_spec] * 2,
            out_specs=(pl.BlockSpec((rows, LANES), lambda c, j, p: (p[j], lead + c)),) * 2,
        ),
        out_shape=finals,
        input_output_aliases={7: 0, 8: 1},
        cost_estimate=cost(bytes_accessed=24 * TAIL * rows * LANES),
    )(place, Og, Ou, xg, xu, yg, yu, fg, fu)
    piece = pl.BlockSpec((1, rows, LANES), lambda c, p: (c, 0, 0))
    fg, fu = pl.pallas_call(
        far_kernel,
        grid_spec=pltpu.PrefetchScalarGridSpec(
            num_scalar_prefetch=1,
            grid=(TAIL,),
            in_specs=[piece] * 2 + [any_spec] * 2,
            out_specs=(pl.BlockSpec((rows, LANES), lambda c, p: (p[3], lead + c)),) * 2,
        ),
        out_shape=finals,
        input_output_aliases={3: 0, 4: 1},
        cost_estimate=cost(bytes_accessed=8 * TAIL * rows * LANES),
    )(place, far_g, far_u, fg, fu)
    return (
        fg, fu, col[:, 0].reshape(width), col[:, 1].reshape(width), N.reshape(4 * ncols * small), rg, ru
    )


def solution(mesh):
    ncols = mesh.shape["cols"]

    def local(*args):
        rows, width = args[0].shape
        if mesh.shape["shard"] == 4 and width % LANES == 0 and rows % 320 == 0 and width // LANES > LAG + TAIL:
            return ringed(*args, ncols)
        return plain(*args)

    return jax.shard_map(
        local,
        mesh=mesh,
        in_specs=(P(("copy", "shard"), "cols"),) * 6 + (P(("copy", "shard", "cols")),) * 2,
        out_specs=(
            P("copy", "cols"),
            P("copy", "cols"),
            P(("copy", "cols")),
            P(("copy", "cols")),
            P("copy"),
            P(("copy", "shard"), "cols"),
            P(("copy", "shard"), "cols"),
        ),
        check_vma=False,
    )
```

```python
import functools

import jax
import jax.numpy as jnp
from jax import lax
from jax.experimental import pallas as pl
from jax.experimental.pallas import tpu as pltpu
from jax.sharding import PartitionSpec as P

learn_rate = 0.015
decay_rate = 0.1
tiny_value = 1e-08
LANES = 128
BLOCK = 64
LAG = 3
TAIL = 5
MESH = pl.DeviceIdType.MESH


def stepped(train, drift, spread):
    return train - learn_rate * (
        drift / (jnp.sqrt(spread) + tiny_value) + decay_rate * train
    )


def plain(
    train_gate, drift_gate, spread_gate, train_up, drift_up, spread_up, norm_train, norm_step
):
    result_gate = stepped(train_gate, drift_gate, spread_gate)
    result_up = stepped(train_up, drift_up, spread_up)
    total_gate, total_up = lax.psum(
        (jnp.sum(result_gate * result_gate, axis=0), jnp.sum(result_up * result_up, axis=0)),
        "shard",
    )
    column_gate = jnp.sqrt(total_gate)
    column_up = jnp.sqrt(total_up)
    narrow_gate = (result_gate / column_gate).astype(jnp.bfloat16)
    narrow_up = (result_up / column_up).astype(jnp.bfloat16)
    final_gate = lax.all_gather(narrow_gate, "shard", axis=0, tiled=True)
    final_up = lax.all_gather(narrow_up, "shard", axis=0, tiled=True)
    serve_norm = lax.all_gather(
        (norm_train + norm_step).astype(jnp.bfloat16), ("shard", "cols"), axis=0, tiled=True
    )
    return (final_gate, final_up, column_gate, column_up, serve_norm, result_gate, result_up)


def gather_kernel(
    chunks, ncols,
    tg, dg, sg, tu, du, su, norm_a, norm_b,
    T, R, Og, Ou, col, N,
    inbuf, res, own, part, gain,
    in_sem, res_sem, loc_sem, tail_sem, psend, precv, osend, orecv, fsend, frecv, nsend, nrecv,
):
    ins = (tg, dg, sg, tu, du, su)
    lead = T.shape[0]
    rows = tg.shape[0]
    me = lax.axis_index("shard")
    mc = lax.axis_index("cols")
    mx = lax.rem(me, 2)
    my = me // 2
    nx = my * 2 + (1 - mx)
    ny = (1 - my) * 2 + mx
    nd = (1 - my) * 2 + (1 - mx)
    peers = (nx, ny, nd)

    def fetch(c, slot):
        return [
            pltpu.make_async_copy(
                ins[k].at[:, pl.ds(pl.multiple_of(c * LANES, LANES), LANES)],
                inbuf.at[slot, k],
                in_sem.at[slot, k],
            )
            for k in range(6)
        ]

    for f in fetch(0, 0):
        f.start()

    everyone = [(i, j) for i in range(4) for j in range(ncols) if i or j]

    def other(i, j):
        return {"shard": lax.rem(me + i, 4), "cols": lax.rem(mc + j, ncols)}

    barrier = pltpu.get_barrier_semaphore()
    for i, j in everyone:
        pl.semaphore_signal(barrier, inc=1, device_id=other(i, j), device_id_type=MESH)
    pl.semaphore_wait(barrier, len(everyone))

    def remote(src, dst, send, recv, shard):
        return pltpu.make_async_remote_copy(
            src_ref=src, dst_ref=dst, send_sem=send, recv_sem=recv,
            device_id={"shard": shard}, device_id_type=MESH,
        )

    def share(c, k):
        return remote(part.at[c, me], part.at[c, me], psend.at[c, k], precv.at[c, k], peers[k])

    def share_in(c, k):
        return remote(part.at[c, peers[k]], part.at[c, peers[k]], psend.at[c, k], precv.at[c, k], peers[k])

    def give(c, k):
        return remote(own.at[c], T.at[c, me], osend.at[c, k], orecv.at[c, k], peers[k])

    def give_in(c, k):
        return remote(own.at[c], T.at[c, peers[k]], osend.at[c, k], orecv.at[c, k], peers[k])

    def pass_on(c, k):
        return remote(
            T.at[c, peers[1 - k], 1 - k], T.at[c, peers[1 - k], 1 - k],
            fsend.at[c, k], frecv.at[c, k], peers[k],
        )

    def pass_in(c, k):
        return remote(
            T.at[c, nd, 1 - k], T.at[c, nd, 1 - k],
            fsend.at[c, k], frecv.at[c, k], peers[k],
        )

    def save(c):
        return pltpu.make_async_copy(res.at[c], R.at[c], res_sem.at[c])

    def keep(c):
        return pltpu.make_async_copy(own.at[c], T.at[c, me], loc_sem.at[c])

    def leave(c):
        return [
            pltpu.make_async_copy(own.at[lead + c, g], out.at[c], tail_sem.at[c, g])
            for g, out in enumerate((Og, Ou))
        ]

    def stage_a(c):
        slot = lax.rem(c, 2)
        for f in fetch(c, slot):
            f.wait()

        @pl.when(c + 1 < chunks)
        def _():
            for f in fetch(c + 1, 1 - slot):
                f.start()

        for g in range(2):
            def body(i, acc):
                at = pl.ds(pl.multiple_of(i * BLOCK, BLOCK), BLOCK)
                value = stepped(
                    inbuf[slot, 3 * g, at, :], inbuf[slot, 3 * g + 1, at, :], inbuf[slot, 3 * g + 2, at, :]
                )
                res[c, g, at, :] = value
                return acc + jnp.sum((value * value).reshape(BLOCK // 8, 8, LANES), axis=0)

            acc = lax.fori_loop(0, rows // BLOCK, body, jnp.zeros((8, LANES), jnp.float32))
            part[c, me, pl.ds(g, 1), :] = jnp.sum(acc, axis=0, keepdims=True)
        for k in range(3):
            share(c, k).start()
        save(c).start()

    def stage_b(c):
        for k in range(3):
            share_in(c, k).wait_recv()
        scale = jnp.sqrt(part[c, 0] + part[c, 1] + part[c, 2] + part[c, 3])
        col[c] = scale
        for g in range(2):
            divisor = scale[g : g + 1, :]

            def body(i, _):
                at = pl.ds(pl.multiple_of(i * BLOCK, BLOCK), BLOCK)
                own[c, g, at, :] = (res[c, g, at, :] / divisor).astype(jnp.bfloat16)
                return 0

            lax.fori_loop(0, rows // BLOCK, body, 0)

        @pl.when(c < lead)
        def _():
            for k in range(2):
                give(c, k).start()
            keep(c).start()

        @pl.when(c >= lead)
        def _():
            for copy in leave(c - lead):
                copy.start()

    def stage_c(c):
        for k in range(2):
            give_in(c, k).wait_recv()
            pass_on(c, 1 - k).start()

    stage_a(0)

    mine = me * ncols + mc
    gain[mine] = (norm_a[...] + norm_b[...]).astype(jnp.bfloat16)

    def gain_copy(n, i, j):
        to = other(i, j)
        return pltpu.make_async_remote_copy(
            src_ref=gain.at[mine], dst_ref=gain.at[mine],
            send_sem=nsend.at[n], recv_sem=nrecv.at[n], device_id=to, device_id_type=MESH,
        )

    def gain_in(n, i, j):
        source = lax.rem(me + 4 - i, 4) * ncols + lax.rem(mc + ncols - j, ncols)
        return pltpu.make_async_remote_copy(
            src_ref=gain.at[source], dst_ref=gain.at[source],
            send_sem=nsend.at[n], recv_sem=nrecv.at[n], device_id=other(i, j), device_id_type=MESH,
        )

    def step(c, _):
        @pl.when(c + 1 < chunks)
        def _():
            stage_a(c + 1)

        stage_b(c)

        @pl.when((c >= LAG) & (c < lead + LAG))
        def _():
            stage_c(c - LAG)

        return 0

    lax.fori_loop(0, chunks, step, 0)
    for n, (i, j) in enumerate(everyone):
        gain_copy(n, i, j).start()
    if lead > chunks - LAG:
        lax.fori_loop(chunks - LAG, lead, lambda c, _: (stage_c(c), 0)[1], 0)

    def settle(c, _):
        for k in range(3):
            share(c, k).wait_send()
        save(c).wait()
        return 0

    def finish(c, _):
        for k in range(2):
            give(c, k).wait_send()
            pass_on(c, k).wait_send()
            pass_in(c, k).wait_recv()
        keep(c).wait()
        return 0

    lax.fori_loop(0, chunks, settle, 0)
    for c in range(chunks - lead):
        for copy in leave(c):
            copy.wait()
    lax.fori_loop(0, lead, finish, 0)
    for n, (i, j) in enumerate(everyone):
        gain_copy(n, i, j).wait_send()
        gain_in(n, i, j).wait_recv()
    N[...] = gain[...]


def lead_kernel(lead, T, fg, fu):
    for c in range(lead):
        at = slice(c * LANES, (c + 1) * LANES)
        fg[:, at] = T[c, 0, 0]
        fu[:, at] = T[c, 0, 1]


def result_kernel(chunks, R, rg, ru):
    for c in range(chunks):
        at = slice(c * LANES, (c + 1) * LANES)
        rg[:, at] = R[c, 0]
        ru[:, at] = R[c, 1]


def near_kernel(place, og, ou, xg, xu, yg, yu, held_g, held_u, fg, fu):
    for j, (gate, up) in enumerate(((og, ou), (xg, xu), (yg, yu))):
        @pl.when(pl.program_id(0) == j)
        def _():
            for c in range(TAIL):
                at = slice(c * LANES, (c + 1) * LANES)
                fg[:, at] = gate[c]
                fu[:, at] = up[c]


def far_kernel(place, g, u, held_g, held_u, fg, fu):
    for c in range(TAIL):
        at = slice(c * LANES, (c + 1) * LANES)
        fg[:, at] = g[c]
        fu[:, at] = u[c]


def ringed(tg, dg, sg, tu, du, su, norm_train, norm_step, ncols):
    rows, width = tg.shape
    chunks = width // LANES
    small = norm_train.shape[0]
    peers = 4 * ncols - 1
    bf16, f32 = jnp.bfloat16, jnp.float32
    dma = pltpu.SemaphoreType.DMA
    any_spec = pl.BlockSpec(memory_space=pl.ANY)
    vmem = pl.BlockSpec(memory_space=pltpu.VMEM)
    lead = chunks - TAIL
    T, R, Og, Ou, col, N = pl.pallas_call(
        functools.partial(gather_kernel, chunks, ncols),
        out_shape=(
            jax.ShapeDtypeStruct((lead, 4, 2, rows, LANES), bf16),
            jax.ShapeDtypeStruct((chunks, 2, rows, LANES), f32),
            jax.ShapeDtypeStruct((TAIL, rows, LANES), bf16),
            jax.ShapeDtypeStruct((TAIL, rows, LANES), bf16),
            jax.ShapeDtypeStruct((chunks, 2, LANES), f32),
            jax.ShapeDtypeStruct((4 * ncols, 1, small), bf16),
        ),
        in_specs=[any_spec] * 6 + [vmem] * 2,
        out_specs=(any_spec,) * 4 + (vmem,) * 2,
        scratch_shapes=[
            pltpu.VMEM((2, 6, rows, LANES), f32),
            pltpu.VMEM((chunks, 2, rows, LANES), f32),
            pltpu.VMEM((chunks, 2, rows, LANES), bf16),
            pltpu.VMEM((chunks, 4, 2, LANES), f32),
            pltpu.VMEM((4 * ncols, 1, small), bf16),
            dma((2, 6)), dma((chunks,)), dma((lead,)), dma((TAIL, 2)),
            dma((chunks, 3)), dma((chunks, 3)),
            dma((lead, 2)), dma((lead, 2)),
            dma((lead, 2)), dma((lead, 2)),
            dma((peers,)), dma((peers,)),
        ],
        compiler_params=pltpu.CompilerParams(
            collective_id=0, has_side_effects=True, vmem_limit_bytes=48 * 2**20
        ),
    )(tg, dg, sg, tu, du, su, norm_train.reshape(1, small), norm_step.reshape(1, small))

    over_x = [(s, s ^ 1) for s in range(4)]
    over_y = [(s, s ^ 2) for s in range(4)]
    xg = lax.ppermute(Og, "shard", over_x)
    yu = lax.ppermute(Ou, "shard", over_y)
    xu = lax.ppermute(Ou, "shard", over_x)
    yg = lax.ppermute(Og, "shard", over_y)

    finals = (jax.ShapeDtypeStruct((4 * rows, width), bf16),) * 2
    results = (jax.ShapeDtypeStruct((rows, width), f32),) * 2
    steps = 5
    block = rows // steps
    cost = functools.partial(pl.CostEstimate, flops=0, transcendentals=0)
    fg, fu = pl.pallas_call(
        functools.partial(lead_kernel, lead),
        grid=(4, steps),
        out_shape=finals,
        in_specs=[pl.BlockSpec((lead, 1, 2, block, LANES), lambda s, r: (0, s, 0, r, 0))],
        out_specs=(pl.BlockSpec((block, lead * LANES), lambda s, r: (s * steps + r, 0)),) * 2,
        cost_estimate=cost(bytes_accessed=32 * lead * rows * LANES),
    )(T)
    xg, yu, fg, fu = lax.optimization_barrier((xg, yu, fg, fu))
    far_g = lax.ppermute(xg, "shard", over_y)
    far_u = lax.ppermute(yu, "shard", over_x)
    thin = rows // 10
    rg, ru = pl.pallas_call(
        functools.partial(result_kernel, chunks),
        grid=(10,),
        out_shape=results,
        in_specs=[pl.BlockSpec((chunks, 2, thin, LANES), lambda r: (0, 0, r, 0))],
        out_specs=(pl.BlockSpec((thin, width), lambda r: (r, 0)),) * 2,
        cost_estimate=cost(bytes_accessed=16 * rows * width),
    )(R)

    me = lax.axis_index("shard")
    place = jnp.stack([me, me ^ 1, me ^ 2, me ^ 3]).astype(jnp.int32)
    half = rows // 2
    wide = (pl.Element(half), pl.Element(TAIL * LANES))

    def source(j):
        return pl.BlockSpec(
            (TAIL, half, LANES),
            lambda i, r, p: (0, jnp.where(i == j, r, jnp.where(i < j, 0, 1)), 0),
        )

    fg, fu = pl.pallas_call(
        near_kernel,
        grid_spec=pltpu.PrefetchScalarGridSpec(
            num_scalar_prefetch=1,
            grid=(3, 2),
            in_specs=[source(j) for j in (0, 0, 1, 1, 2, 2)] + [any_spec] * 2,
            out_specs=(
                pl.BlockSpec(wide, lambda i, r, p: ((p[i] * 2 + r) * half, lead * LANES)),
            ) * 2,
        ),
        out_shape=finals,
        input_output_aliases={7: 0, 8: 1},
        cost_estimate=cost(bytes_accessed=24 * TAIL * rows * LANES),
    )(place, Og, Ou, xg, xu, yg, yu, fg, fu)
    piece = pl.BlockSpec((TAIL, half, LANES), lambda r, p: (0, r, 0))
    fg, fu = pl.pallas_call(
        far_kernel,
        grid_spec=pltpu.PrefetchScalarGridSpec(
            num_scalar_prefetch=1,
            grid=(2,),
            in_specs=[piece] * 2 + [any_spec] * 2,
            out_specs=(
                pl.BlockSpec(wide, lambda r, p: ((p[3] * 2 + r) * half, lead * LANES)),
            ) * 2,
        ),
        out_shape=finals,
        input_output_aliases={3: 0, 4: 1},
        cost_estimate=cost(bytes_accessed=8 * TAIL * rows * LANES),
    )(place, far_g, far_u, fg, fu)
    return (
        fg, fu, col[:, 0].reshape(width), col[:, 1].reshape(width), N.reshape(4 * ncols * small), rg, ru
    )


def solution(mesh):
    ncols = mesh.shape["cols"]

    def local(*args):
        rows, width = args[0].shape
        if mesh.shape["shard"] == 4 and width % LANES == 0 and rows % 320 == 0 and width // LANES > LAG + TAIL:
            return ringed(*args, ncols)
        return plain(*args)

    return jax.shard_map(
        local,
        mesh=mesh,
        in_specs=(P(("copy", "shard"), "cols"),) * 6 + (P(("copy", "shard", "cols")),) * 2,
        out_specs=(
            P("copy", "cols"),
            P("copy", "cols"),
            P(("copy", "cols")),
            P(("copy", "cols")),
            P("copy"),
            P(("copy", "shard"), "cols"),
            P(("copy", "shard"), "cols"),
        ),
        check_vma=False,
    )
```
